512 devices in a mesh: dp: 32 (over y, z_lo), mp: 16 (over x, z_hi, core).
Axes of the slice: x: 4, y: 4, z: 16 (z_hi: 2, z_lo: 8; z = z_hi * 8 + z_lo), core: 2. Of those that a mesh axis runs over, the one named last changes fastest.
Arguments:
- logits: bfloat16 [4096, 65536], P('dp', 'mp'), may hold values from -72 to 240
- targets: int32 [4096], P('dp'), may hold values from 0 to 65535
- resp_mask: int32 [4096], P('dp'), may hold values from 0 to 1, as said below
- rewards: int32 [32], P('dp'), may hold values from 0 to 10
- groups: int32 [32], P('dp'), may hold values from 0 to 7, as said below
- unit_grad: bfloat16 [4096, 8192], P(('dp', 'mp')), may hold values from -192 to 192
- mix: bfloat16 [4096, 8192], P('dp', 'mp'), may hold values from -6 to 6
- w_out: bfloat16 [8192, 8192], P('mp', 'dp'), may hold values from -0.0625 to 0.0625
Outputs:
- token_logprob: float32 [4096], P('dp')
- policy_loss: float32 [], replicated
- grad_mix: bfloat16 [4096, 8192], P('dp', 'mp')
- grad_w_out: bfloat16 [8192, 8192], P('mp', 'dp')
The draws below stay inside these ranges and needn't reach their ends.
Inputs may be any that keep to these rules, and one draw needn't show every extreme that they name: `resp_mask`: in each sample the response mask is a run of ones followed by zeros, with at least 32 ones. `groups`: each prompt id names exactly 4 samples.
All inputs are finite; a program needn't handle non-finite values.
Results may differ from the reference program's by a relative error of at most 0.005.
Values may be sent and summed in bfloat16 or wider, within the bound.
A program may use at most 64 MiB of HBM per device.

```python
import jax
import jax.numpy as jnp
from jax import lax

D = 8192
K = 4
ROWS = 128
SEQS = 32
PROMPTS = 8
TOKENS = 4096
VOCAB = 65536
QW = 8192


def draw_logits(key, part):
    keys = jax.random.split(key, 1)
    values = 3.0 * jnp.clip(jax.random.normal(keys[0], (TOKENS, VOCAB), jnp.float32), -6.0, 6.0)
    return values.astype(jnp.bfloat16)


def draw_resp_mask(key, part):
    jitter = jax.random.randint(key, (SEQS, 1), 0, ROWS // 8 + 1)
    sample_index = jnp.arange(SEQS, dtype=jnp.int32)[:, None]
    length = jnp.minimum(ROWS // 4 + sample_index * (ROWS * 3 // 4) // SEQS + jitter, ROWS)
    position = jnp.arange(ROWS, dtype=jnp.int32)[None, :]
    return (position < length).astype(jnp.int32).reshape(TOKENS)


def draw_groups(key, part):
    return (jax.random.permutation(key, SEQS) // K).astype(jnp.int32)


def touch_ends(values, key, least, top_value):
    extent = values.shape
    place = [jax.random.randint(jax.random.fold_in(key, axis), (), 0, extent[axis]) for axis in range(len(extent))]
    values = values.at[tuple(place)].set(least)
    longest = extent.index(max(extent))
    place[longest] = (place[longest] + 1) % extent[longest]
    return values.at[tuple(place)].set(top_value)


def block_scale(own_key, shape, pieces, least, high):
    def one(dim, blocks):
        draws = jax.random.uniform(jax.random.fold_in(jax.random.fold_in(own_key, 6), dim), (blocks,), jnp.float32, least / len(pieces), high / len(pieces))
        return jnp.repeat(jnp.exp(draws), shape[dim] // blocks).reshape((-1,) + (1,) * (len(shape) - dim - 1))

    factor_of = one(*pieces[0])
    for cut in pieces[1:]:
        factor_of = factor_of * one(*cut)
    return factor_of


def gaussian(key, dims, width, reach, cuts=(), kind=jnp.bfloat16):
    level = block_scale(key, dims, cuts, -0.22, 0.18) if cuts else 1.0
    array = jax.random.normal(key, dims, jnp.float32) * width * level
    return jnp.minimum(jnp.maximum(array, -reach), reach).astype(kind)


def setup_inputs(seed: int = 0) -> dict:
    key_of = jax.random.split(jax.random.key(seed), 9)
    logits = draw_logits(jax.random.fold_in(key_of[8], 71), 0)
    targets = touch_ends(jax.random.randint(key_of[1], (TOKENS,), 0, VOCAB), jax.random.fold_in(key_of[1], 1), 0, VOCAB - 1).astype(jnp.int32)
    resp_mask = draw_resp_mask(jax.random.fold_in(key_of[8], 71), 0)
    rewards = touch_ends(jax.random.randint(key_of[3], (SEQS,), 0, 11), jax.random.fold_in(key_of[3], 1), 0, 10).astype(jnp.int32)
    groups = draw_groups(jax.random.fold_in(key_of[8], 71), 0)
    unit_grad = gaussian(key_of[5], (TOKENS, D), 32.0, 192.0, ((0, 512),))
    mix = gaussian(key_of[6], (TOKENS, QW), 1.0, 6.0, ((0, 32), (1, 16)))
    w_out = gaussian(key_of[7], (QW, D), QW ** -0.5, 0.0625, ((0, 16), (1, 32)))
    return {"logits": logits, "targets": targets, "resp_mask": resp_mask, "rewards": rewards, "groups": groups, "unit_grad": unit_grad, "mix": mix, "w_out": w_out}


def sample_logprob(inputs):
    values, chosen = inputs
    wide = values.astype(jnp.float32)
    highest = jnp.max(wide, axis=1)
    summed = jnp.sum(jnp.exp(wide - highest[:, None]), axis=1)
    picked = jnp.take_along_axis(wide, chosen[:, None].astype(jnp.int32), axis=1)[:, 0]
    return picked - (highest + jnp.log(summed))


def reference(logits, targets, resp_mask, rewards, groups, unit_grad, mix, w_out):
    logprob = lax.map(sample_logprob, (logits.reshape(SEQS, ROWS, VOCAB), targets.reshape(SEQS, ROWS)))
    mask_float = resp_mask.astype(jnp.float32).reshape(SEQS, ROWS)
    token_count = jnp.sum(mask_float)
    reward_float = rewards.astype(jnp.float32)
    member = (groups[:, None] == jnp.arange(PROMPTS, dtype=jnp.int32)[None, :]).astype(jnp.float32)
    group_total = jnp.sum(member * reward_float[:, None], axis=0)
    own_total = jnp.sum(member * group_total[None, :], axis=1)
    advantage = reward_float - (own_total - reward_float) / (K - 1)
    weight = advantage[:, None] * mask_float / token_count
    policy_loss = -jnp.sum(weight * logprob)
    grad_out = (-weight.reshape(TOKENS)[:, None] * unit_grad.astype(jnp.float32)).astype(jnp.bfloat16)
    grad_mix = jnp.dot(grad_out, w_out.T, preferred_element_type=jnp.float32).astype(jnp.bfloat16)
    grad_w_out = jnp.dot(mix.T, grad_out, preferred_element_type=jnp.float32).astype(jnp.bfloat16)
    return logprob.reshape(TOKENS), policy_loss, grad_mix, grad_w_out
```

```python
import jax
import jax.numpy as jnp
from jax import lax
from jax.sharding import Mesh
from jax.sharding import PartitionSpec as P

K = 4
Y, Z = "dp_0", "dp_1"
DP = (Y, Z)
DP_MP = (Y, Z, "mp")


def shards(logits, targets, resp_mask, rewards, groups, unit_grad, mix, w_out):
    rows, vocab = logits.shape
    lane = lax.axis_index("mp")
    ny, nz, nmp = lax.axis_size(Y), lax.axis_size(Z), lax.axis_size("mp")
    wide = logits.astype(jnp.float32)
    local_target = targets - lane * vocab
    hit = lax.broadcasted_iota(jnp.int32, logits.shape, 1) == local_target[:, None]
    picked = jnp.sum(jnp.where(hit, wide, 0.0), axis=1)
    local_max = jnp.max(wide, axis=1)
    local_sum = jnp.sum(jnp.exp(wide - local_max[:, None]), axis=1)
    stats = lax.all_gather(jnp.stack([local_max, local_sum, picked]), "mp")
    top = jnp.max(stats[:, 0], axis=0)
    total = jnp.sum(stats[:, 1] * jnp.exp(stats[:, 0] - top), axis=0)
    logprob = jnp.sum(stats[:, 2], axis=0) - (top + jnp.log(total))

    length = jnp.sum(resp_mask)
    info = jnp.stack([rewards[0], groups[0], length]).astype(jnp.float32)
    every = lax.all_gather(info, DP)
    reward, group, count = every[:, 0], every[:, 1], every[:, 2]
    same = (group[:, None] == group[None, :]).astype(jnp.float32)
    own_total = jnp.sum(same * reward[None, :], axis=1)
    scale = (reward - (own_total - reward) / (K - 1)) / jnp.sum(count)
    token_count = jnp.sum(count)
    advantage = reward - (own_total - reward) / (K - 1)
    me = lax.axis_index(Y) * nz + lax.axis_index(Z)
    mask = resp_mask.astype(jnp.float32)
    weight = advantage[me] * mask / token_count
    policy_loss = jnp.sum(lax.all_gather(-jnp.sum(weight * logprob), DP))

    sub = unit_grad.shape[0]
    part = lax.dynamic_slice_in_dim(weight, lane * sub, sub)
    grad = (-part[:, None] * unit_grad.astype(jnp.float32)).astype(jnp.bfloat16)
    depth = w_out.shape[1]
    grad = grad.reshape(sub, ny, nz, depth).transpose(2, 0, 1, 3).reshape(nz, sub, ny * depth)
    grad = lax.all_to_all(grad, Z, 0, 0, tiled=True)
    grad = lax.all_gather(grad, "mp", axis=1, tiled=True).reshape(nz * rows, ny * depth)
    w_cols = lax.all_gather(w_out, Y, axis=1, tiled=True)
    mix_rows = lax.all_gather(mix, Z, axis=0, tiled=True)
    part_mix = lax.dot_general(
        grad, w_cols, (((1,), (1,)), ((), ())), preferred_element_type=jnp.float32
    ).astype(jnp.bfloat16)
    grad_mix = lax.psum_scatter(part_mix, Z, scatter_dimension=0, tiled=True)
    part_w = lax.dot_general(
        mix_rows, grad, (((0,), (0,)), ((), ())), preferred_element_type=jnp.float32
    ).astype(jnp.bfloat16)
    grad_w_out = lax.psum_scatter(part_w, Y, scatter_dimension=1, tiled=True)
    return logprob, policy_loss, grad_mix, grad_w_out


def solution(mesh):
    finer = Mesh(mesh.devices.reshape(4, 8, mesh.shape["mp"]), ("dp_0", "dp_1", "mp"))
    in_specs = (P(DP, "mp"), P(DP), P(DP), P(DP), P(DP), P(DP_MP, None), P(DP, "mp"), P("mp", DP))
    out_specs = (P(DP), P(), P(DP, "mp"), P("mp", DP))
    return jax.shard_map(
        shards, mesh=finer, in_specs=in_specs, out_specs=out_specs, check_vma=False
    )
```

```python
import jax
import jax.numpy as jnp
from jax import lax
from jax.experimental import pallas as pl
from jax.experimental.pallas import tpu as pltpu
from jax.sharding import Mesh
from jax.sharding import PartitionSpec as P

K = 4
NY, NZ, NX = 4, 8, 4
DP = ("y", "zl")
MP = ("x", "zh", "core")
F32, BF16 = jnp.float32, jnp.bfloat16
NT = (((1,), (1,)), ((), ()))
TN = (((0,), (0,)), ((), ()))
SUB = 4


def kernel(
    logits, targets, mask, rewards, groups, ug, mix, w_out,
    lp_out, loss_out, gmix_out, gw_out,
    LG, US, GR, MX, W, G2, PF, RB, SB, GW, YS, YR, INFO, WSC, LSC, STA, STB, LZ, LY,
    lsem, zsem, xsem, dsem, msem, wsem, rsem, ysem, ssem, mssem, sends,
):
    y, k, x = lax.axis_index("y"), lax.axis_index("zl"), lax.axis_index("x")
    h, c = lax.axis_index("zh"), lax.axis_index("core")
    rows, vocab = LG.shape
    depth = W.shape[2]
    xr, xl = lax.rem(x + 1, NX), lax.rem(x + NX - 1, NX)
    xo = lax.rem(x + 2, NX)
    yr, yl = lax.rem(y + 1, NY), lax.rem(y + NY - 1, NY)
    yo = lax.rem(y + 2, NY)
    right, left, opp = {"zl": k + 1}, {"zl": k - 1}, {"core": 1 - c}

    def idx(xx, cc, zz, hh):
        return ((xx * 2 + cc) * NZ + zz) * 2 + hh

    def unit(xx, cc, zz):
        return GR.at[pl.ds(idx(xx, cc, zz, 0), 2)]

    def put(src, dst, send, recv, where):
        pltpu.make_async_remote_copy(
            src_ref=src, dst_ref=dst, send_sem=send, recv_sem=recv,
            device_id=where, device_id_type=pl.DeviceIdType.MESH,
        ).start()

    def take(ref, sem):
        pltpu.make_async_copy(ref, ref, sem).wait()

    def cols(i):
        return pl.ds(pl.multiple_of(i * depth, depth), depth)

    load_logits = pltpu.make_async_copy(logits, LG, lsem.at[0])
    load_logits.start()
    for yy in range(NY):
        for zz in range(NZ):
            pltpu.make_async_copy(
                ug.at[:, pl.ds((yy * NZ + zz) * depth, depth)],
                US.at[zz, :, pl.ds(yy * depth, depth)], lsem.at[1],
            ).start()
    for yy in range(NY):
        pltpu.make_async_copy(
            ug.at[:, cols(yy * NZ + k)],
            GR.at[idx(x, c, k, h), :, pl.ds(yy * depth, depth)], zsem.at[k],
        ).start()
    own_rows = pl.ds(pl.multiple_of(k * rows, rows), rows)
    for q in range(SUB):
        pltpu.make_async_copy(
            mix.at[:, pl.ds(q * 128, 128)], MX.at[q, own_rows], lsem.at[2]
        ).start()
    load_w = pltpu.make_async_copy(w_out, W.at[y], lsem.at[3])
    load_w.start()

    barrier = pltpu.get_barrier_semaphore()
    peers = []
    for step in range(1, 2 * NZ):
        place = lax.rem(h * NZ + k + step, 2 * NZ)
        peers.append({"zh": place // NZ, "zl": lax.rem(place, NZ)})
    peers += [{"y": lax.rem(y + i, NY)} for i in range(1, NY)]
    peers += [{"x": lax.rem(x + i, NX)} for i in range(1, NX)]
    peers += [opp, {"zh": 1 - h, "core": 1 - c}]
    for peer in peers:
        pl.semaphore_signal(barrier, inc=1, device_id=peer, device_id_type=pl.DeviceIdType.MESH)

    lane = lax.broadcasted_iota(jnp.int32, (1, 128), 1)
    length = jnp.sum(mask[...].astype(F32), axis=1, keepdims=True)
    facts = jnp.where(lane == 0, rewards[0].astype(F32), 0.0)
    facts = facts + jnp.where(lane == 1, groups[0].astype(F32), 0.0)
    facts = facts + jnp.where(lane == 2, jnp.broadcast_to(length, (1, 128)), 0.0)
    INFO[y * NZ + k] = facts

    load_logits.wait()
    eye = lax.broadcasted_iota(jnp.int32, (rows, rows), 0) == lax.broadcasted_iota(
        jnp.int32, (rows, rows), 1
    )
    column = lax.broadcasted_iota(jnp.int32, (rows, 128), 1).astype(F32)
    shift = ((x * 2 + h) * 2 + c) * vocab
    wanted = (targets[...] - shift).astype(F32)
    wanted = jnp.sum(jnp.where(eye, wanted, 0.0), axis=1, keepdims=True)

    def piece(j):
        return LG[:, pl.ds(pl.multiple_of(j * 128, 128), 128)].astype(F32)

    tiles = vocab // 128
    peak = lax.fori_loop(
        0, tiles, lambda j, m: jnp.maximum(m, piece(j)), jnp.full((rows, 128), -jnp.inf, F32)
    )
    peak = jnp.max(peak, axis=1, keepdims=True)

    def collect(j, carry):
        total, found = carry
        value = piece(j)
        total = total + jnp.exp(value - peak)
        at = wanted - (j * 128).astype(F32)
        return total, found + jnp.where(column == at, value, 0.0)

    zero = jnp.zeros((rows, 128), F32)
    total, found = lax.fori_loop(0, tiles, collect, (zero, zero))

    def as_row(v):
        return jnp.sum(jnp.where(eye, v, 0.0), axis=0, keepdims=True)

    a = h * 2 + c
    STA[a, 0:1, :] = as_row(peak)
    STA[a, 1:2, :] = as_row(jnp.sum(total, axis=1, keepdims=True))
    STA[a, 2:3, :] = as_row(jnp.sum(found, axis=1, keepdims=True))

    for ref, sem in ((US, lsem.at[1]), (MX.at[:, own_rows], lsem.at[2])):
        take(ref, sem)
    load_w.wait()
    pl.semaphore_wait(barrier, len(peers))

    me = y * NZ + k
    for i in range(1, NZ):
        to = lax.rem(k + i, NZ)
        put(INFO.at[me], INFO.at[me], sends.at[0], ssem.at[0], {"zl": to})
    mine = idx(x, c, k, h)
    for far in range(NZ - 1, -1, -1):
        for side in (1, -1) if far else (1,):
            to = k + side * far

            def send_rows(to=to, far=far):
                for hh in (0, 1):
                    if far == 0 and hh == 0:
                        continue
                    zh = hh if far else 1 - h
                    put(US.at[to], GR.at[mine], sends.at[1], zsem.at[k], {"zl": to, "zh": zh})

            if far == 0:
                send_rows()
            else:
                pl.when((to >= 0) & (to < NZ))(send_rows)
    half = W.shape[1] // 2
    first, second = pl.ds(0, half), pl.ds(half, half)
    put(W.at[y, first], W.at[y, first], sends.at[2], wsem.at[0], {"y": yr})
    put(W.at[y, second], W.at[y, second], sends.at[2], wsem.at[3], {"y": yl})
    put(W.at[y, second], W.at[y, second], sends.at[2], wsem.at[1], {"y": yr})
    put(W.at[y, first], W.at[y, first], sends.at[2], wsem.at[4], {"y": yl})

    def mix_at(zz, q):
        return MX.at[q, pl.ds(pl.multiple_of(zz * rows, rows), rows)]

    def mix_hop(hop, waiting):
        def one(q, carry):
            for side, away, ok in ((0, -1, k < NZ - 1), (1, 1, k > 0)):
                origin = k + away * hop

                def forward(side=side, origin=origin, ok=ok):
                    if waiting:
                        take(mix_at(origin, q), msem.at[origin, q])

                    @pl.when(ok)
                    def _():
                        put(
                            mix_at(origin, q), mix_at(origin, q), mssem.at[side, hop],
                            msem.at[origin, q], (right, left)[side],
                        )

                pl.when((origin >= 0) & (origin < NZ))(forward)
            return carry

        lax.fori_loop(0, SUB, one, 0)

    mix_hop(0, False)
    for peer in ({"zh": 1 - h}, opp, {"zh": 1 - h, "core": 1 - c}):
        put(STA.at[a], STA.at[a], sends.at[3], ssem.at[2], peer)

    take(INFO.at[pl.ds(0, NZ - 1)], ssem.at[0])
    line = INFO.at[pl.ds(y * NZ, NZ)]
    for i in range(1, NY):
        put(line, line, sends.at[4], ssem.at[1], {"y": lax.rem(y + i, NY)})

    take(W.at[yl, first], wsem.at[0])
    put(W.at[yl, first], W.at[yl, first], sends.at[5], wsem.at[2], {"y": yr})
    take(W.at[yr, second], wsem.at[3])
    put(W.at[yr, second], W.at[yr, second], sends.at[5], wsem.at[5], {"y": yl})

    take(INFO.at[pl.ds(0, (NY - 1) * NZ)], ssem.at[1])
    count = jnp.zeros((1, 128), F32)
    for r in range(NY * NZ):
        count = count + INFO[r]
    count = jnp.broadcast_to(count[:, 2:3], (1, 128))

    def weigh(zz, carry):
        fact = INFO[y * NZ + zz]
        reward = jnp.broadcast_to(fact[:, 0:1], (1, 128))
        group = jnp.broadcast_to(fact[:, 1:2], (1, 128))
        own = jnp.zeros((1, 128), F32)
        for r in range(NY * NZ):
            other = INFO[r]
            same = jnp.broadcast_to(other[:, 1:2], (1, 128)) == group
            own = own + jnp.where(same, jnp.broadcast_to(other[:, 0:1], (1, 128)), 0.0)
        WSC[zz] = (reward - (own - reward) / (K - 1)) / count
        LSC[zz] = jnp.broadcast_to(fact[:, 2:3], (1, 128))
        return carry

    lax.fori_loop(0, NZ, weigh, 0)

    def merge(ref, n):
        top = ref[0, 0:1, :]
        for i in range(1, n):
            top = jnp.maximum(top, ref[i, 0:1, :])
        total = jnp.zeros_like(top)
        found = jnp.zeros_like(top)
        for i in range(n):
            total = total + ref[i, 1:2, :] * jnp.exp(ref[i, 0:1, :] - top)
            found = found + ref[i, 2:3, :]
        return top, total, found

    take(STA.at[pl.ds(0, 3)], ssem.at[2])
    for i, v in enumerate(merge(STA, 4)):
        STB[x, i : i + 1, :] = v

    def arrived(zz):
        take(unit(x, c, zz), zsem.at[zz])
        here = unit(x, c, zz)
        put(here, here, sends.at[6], xsem.at[0, zz], {"x": xr})
        put(here, here, sends.at[6], xsem.at[1, zz], {"x": xl})
        put(here, here, sends.at[7], dsem.at[zz], opp)

    def passed(zz):
        for side, origin, to in ((0, xl, xr), (1, xr, xl)):
            here = unit(origin, c, zz)
            take(here, xsem.at[side, zz])
            part = GR.at[idx(origin, c, zz, side)]
            put(part, part, sends.at[6], xsem.at[2 + side, zz], {"x": to})
            put(here, here, sends.at[7], dsem.at[zz], opp)

    def closed(zz):
        for side in (0, 1):
            take(GR.at[idx(xo, c, zz, side)], xsem.at[2 + side, zz])
        here = unit(xo, c, zz)
        put(here, here, sends.at[7], dsem.at[zz], opp)

    def partial(zz):
        take(GR.at[pl.ds(0, 8)], dsem.at[zz])
        weight, limit = WSC[zz], LSC[zz]
        base = pl.multiple_of(zz * rows, rows)

        def scale(i, carry):
            xx, hh = i // 2, lax.rem(i, 2)
            pair = jnp.concatenate(
                [GR[idx(xx, cc, zz, hh)].astype(F32) for cc in (0, 1)], axis=0
            )
            place = (lax.broadcasted_iota(jnp.int32, (16, 128), 0) + i * 16).astype(F32)
            factor = jnp.where(place < limit, -weight, 0.0)
            factor = jnp.concatenate([factor] * (pair.shape[1] // 128), axis=1)
            G2[pl.ds(pl.multiple_of(base + i * 16, 16), 16), :] = (factor * pair).astype(BF16)
            return carry

        lax.fori_loop(0, rows // 16, scale, 0)
        block = G2[pl.ds(base, rows), :]
        acc = None
        for yy in range(NY):
            one = lax.dot_general(
                block[:, yy * depth : (yy + 1) * depth], W[yy], NT, preferred_element_type=F32
            )
            acc = one if acc is None else acc + one
        PF[zz] = acc

    def both(far, act):
        for side in (1, -1):
            zz = k + side * far
            ok = (zz >= 0) & (zz < NZ) & (far >= 0) & (far < NZ)
            if side == -1:
                ok = ok & (far > 0)

            pl.when(ok)(lambda zz=zz: act(zz))

    step_rows = rows // SUB

    def scatter_slot(s):
        going = ((0, NZ - 1 - (s - k), s >= k, k > 0), (1, s - (NZ - 1 - k), s >= NZ - 1 - k, k < NZ - 1))

        def one(q, carry):
            part = pl.ds(pl.multiple_of(q * step_rows, step_rows), step_rows)
            for side, to, ok, more in going:

                def store(side=side, to=to, more=more):
                    @pl.when(more)
                    def _():
                        take(RB.at[side, to, part], rsem.at[side, to, q])
                        SB[to, part, :] = (PF[to, part, :] + RB[side, to, part, :].astype(F32)).astype(BF16)

                    @pl.when(jnp.logical_not(more))
                    def _():
                        SB[to, part, :] = PF[to, part, :].astype(BF16)

                pl.when(ok)(store)
            for side, to, ok, more in going:

                def send(side=side, to=to):
                    put(
                        SB.at[to, part], RB.at[side, to, part], sends.at[8],
                        rsem.at[side, to, q], (right, left)[side],
                    )

                pl.when(ok)(send)
            return carry

        lax.fori_loop(0, SUB, one, 0)

    for i in range(1, NX):
        put(STB.at[x], STB.at[x], sends.at[9], ssem.at[3], {"x": lax.rem(x + i, NX)})

    def step(t, carry):
        pl.when(t < NZ - 1)(lambda: mix_hop(t + 1, True))
        both(NZ - 1 - t, arrived)
        both(NZ - t, passed)
        both(NZ + 1 - t, closed)

        @pl.when(t == 2)
        def _():
            take(W.at[yl, second], wsem.at[1])
            take(W.at[yr, first], wsem.at[4])
            take(W.at[yo, first], wsem.at[2])
            take(W.at[yo, second], wsem.at[5])

        both(NZ + 2 - t, partial)
        pl.when((t >= 3) & (t < NZ + 2))(lambda: scatter_slot(t - 3))
        return carry

    lax.fori_loop(0, NZ + 3, step, 0)

    take(STB.at[pl.ds(0, NX - 1)], ssem.at[3])
    top, total, found = merge(STB, NX)
    logprob = found - (top + jnp.log(total))
    lp_out[...] = logprob
    weight = jnp.where(lane.astype(F32) < LSC[k], WSC[k], 0.0)
    LZ[k] = jnp.broadcast_to(-jnp.sum(weight * logprob, axis=1, keepdims=True), (1, 128))

    def product(q):
        GW[q] = lax.dot_general(MX[q], G2[...], TN, preferred_element_type=F32)

    def stage(slot, value):
        YS[slot] = value.astype(BF16)

    product(0)
    for i in range(1, NZ):
        put(LZ.at[k], LZ.at[k], sends.at[10], ssem.at[4], {"zl": lax.rem(k + i, NZ)})
    stage(0, GW[0, :, cols(yo)])
    product(2)
    put(YS.at[0], YR.at[0], sends.at[11], ysem.at[0], {"y": yr})
    stage(6, GW[2, :, cols(yo)])
    product(1)
    put(YS.at[6], YR.at[6], sends.at[11], ysem.at[6], {"y": yl})
    stage(1, GW[1, :, cols(yo)])
    stage(10, GW[0, :, cols(yl)])
    product(3)
    put(YS.at[1], YR.at[1], sends.at[11], ysem.at[1], {"y": yr})
    put(YS.at[10], YR.at[10], sends.at[11], ysem.at[10], {"y": yl})
    stage(7, GW[3, :, cols(yo)])
    stage(4, GW[2, :, cols(yr)])
    stage(5, GW[3, :, cols(yr)])
    stage(11, GW[1, :, cols(yl)])
    put(YS.at[7], YR.at[7], sends.at[11], ysem.at[7], {"y": yl})
    put(YS.at[4], YR.at[4], sends.at[11], ysem.at[4], {"y": yr})
    put(YS.at[11], YR.at[11], sends.at[11], ysem.at[11], {"y": yl})
    put(YS.at[5], YR.at[5], sends.at[11], ysem.at[5], {"y": yr})

    acc = PF[k]
    gmix_out[...] = acc.astype(BF16)
    for side, more in ((0, k > 0), (1, k < NZ - 1)):

        @pl.when(more)
        def _(side=side):
            for q in range(SUB):
                part = pl.ds(q * step_rows, step_rows)
                take(RB.at[side, k, part], rsem.at[side, k, q])
            PF[k] = PF[k] + RB[side, k].astype(F32)

    gmix_out[...] = PF[k].astype(BF16)

    take(LZ.at[pl.ds(0, NZ - 1)], ssem.at[4])
    LY[y] = jnp.sum(LZ[...], axis=0)

    for i in (0, 1):
        take(YR.at[i], ysem.at[i])
        stage(2 + i, GW[i, :, cols(yr)] + YR[i].astype(F32))
        take(YR.at[6 + i], ysem.at[6 + i])
        stage(8 + i, GW[2 + i, :, cols(yl)] + YR[6 + i].astype(F32))
        put(YS.at[2 + i], YR.at[2 + i], sends.at[11], ysem.at[2 + i], {"y": yr})
        put(YS.at[8 + i], YR.at[8 + i], sends.at[11], ysem.at[8 + i], {"y": yl})
    for i in range(1, NY):
        put(LY.at[y], LY.at[y], sends.at[12], ssem.at[5], {"y": lax.rem(y + i, NY)})
    for q, (one, two) in enumerate(((2, 10), (3, 11), (8, 4), (9, 5))):
        take(YR.at[one], ysem.at[one])
        take(YR.at[two], ysem.at[two])
        value = GW[q, :, cols(y)] + YR[one].astype(F32) + YR[two].astype(F32)
        gw_out[pl.ds(q * 128, 128), :] = value.astype(BF16)

    take(LY.at[pl.ds(0, NY - 1)], ssem.at[5])
    loss_out[0, 0] = jnp.sum(jnp.sum(LY[...], axis=0)[:, 0:1])

    take(INFO.at[pl.ds(0, NZ - 1)], sends.at[0])
    take(GR.at[pl.ds(0, 2 * NZ - 1)], sends.at[1])
    take(W.at[pl.ds(0, 2)], sends.at[2])
    take(STA.at[pl.ds(0, 3)], sends.at[3])
    take(INFO.at[pl.ds(0, (NY - 1) * NZ)], sends.at[4])
    take(W.at[0], sends.at[5])
    take(GR.at[pl.ds(0, 6 * NZ)], sends.at[6])
    take(GR.at[pl.ds(0, 8 * NZ)], sends.at[7])
    take(SB.at[pl.ds(0, NZ - 1)], sends.at[8])
    take(STB.at[pl.ds(0, NX - 1)], sends.at[9])
    take(LZ.at[pl.ds(0, NZ - 1)], sends.at[10])
    take(YR, sends.at[11])
    take(LY.at[pl.ds(0, NY - 1)], sends.at[12])
    for side, away, ok in ((0, -1, k < NZ - 1), (1, 1, k > 0)):
        for hop in range(NZ):
            origin = k + away * hop
            pl.when((origin >= 0) & (origin < NZ) & ok)(
                lambda side=side, hop=hop: take(MX.at[:, pl.ds(0, rows)], mssem.at[side, hop])
            )


def shards(logits, targets, resp_mask, rewards, groups, unit_grad, mix, w_out):
    rows, vocab = logits.shape
    heads, depth = w_out.shape
    sub = unit_grad.shape[0]
    vmem = pl.BlockSpec(memory_space=pltpu.VMEM)
    smem = pl.BlockSpec(memory_space=pltpu.SMEM)
    hbm = pl.BlockSpec(memory_space=pltpu.HBM)
    dma = pltpu.SemaphoreType.DMA
    logprob, loss, grad_mix, grad_w = pl.pallas_call(
        kernel,
        name="step",
        out_shape=(
            jax.ShapeDtypeStruct((1, rows), F32),
            jax.ShapeDtypeStruct((1, 1), F32),
            jax.ShapeDtypeStruct((rows, heads), BF16),
            jax.ShapeDtypeStruct((heads, depth), BF16),
        ),
        in_specs=[hbm, vmem, vmem, smem, smem, hbm, hbm, hbm],
        out_specs=(vmem, smem, vmem, vmem),
        scratch_shapes=[
            pltpu.VMEM((rows, vocab), BF16),
            pltpu.VMEM((NZ, sub, NY * depth), BF16),
            pltpu.VMEM((NX * 2 * NZ * 2, sub, NY * depth), BF16),
            pltpu.VMEM((SUB, NZ * rows, heads // SUB), BF16),
            pltpu.VMEM((NY, heads, depth), BF16),
            pltpu.VMEM((NZ * rows, NY * depth), BF16),
            pltpu.VMEM((NZ, rows, heads), F32),
            pltpu.VMEM((2, NZ, rows, heads), BF16),
            pltpu.VMEM((NZ, rows, heads), BF16),
            pltpu.VMEM((SUB, heads // SUB, NY * depth), F32),
            pltpu.VMEM((12, heads // SUB, depth), BF16),
            pltpu.VMEM((12, heads // SUB, depth), BF16),
            pltpu.VMEM((NY * NZ, 1, 128), F32),
            pltpu.VMEM((NZ, 1, 128), F32),
            pltpu.VMEM((NZ, 1, 128), F32),
            pltpu.VMEM((4, 8, 128), F32),
            pltpu.VMEM((NX, 8, 128), F32),
            pltpu.VMEM((NZ, 1, 128), F32),
            pltpu.VMEM((NY, 1, 128), F32),
            dma((4,)), dma((NZ,)), dma((4, NZ)), dma((NZ,)), dma((NZ, SUB)), dma((6,)),
            dma((2, NZ, SUB)), dma((12,)), dma((6,)), dma((2, NZ)), dma((13,)),
        ],
        compiler_params=pltpu.CompilerParams(
            collective_id=0, has_side_effects=True, vmem_limit_bytes=58 * 1024 * 1024
        ),
    )(
        logits, targets.reshape(1, rows), resp_mask.reshape(1, rows), rewards, groups,
        unit_grad, mix, w_out,
    )
    return logprob.reshape(rows), loss.reshape(()), grad_mix, grad_w


def solution(mesh):
    finer = Mesh(mesh.devices.reshape(NY, NZ, NX, 2, 2), DP + MP)
    in_specs = (
        P(DP, MP), P(DP), P(DP), P(DP), P(DP), P(DP + MP, None), P(DP, MP), P(MP, DP)
    )
    out_specs = (P(DP), P(), P(DP, MP), P(MP, DP))
    return jax.shard_map(
        shards, mesh=finer, in_specs=in_specs, out_specs=out_specs, check_vma=False
    )
```

```python
import jax
import jax.numpy as jnp
from jax import lax
from jax.experimental import pallas as pl
from jax.experimental.pallas import tpu as pltpu
from jax.sharding import Mesh
from jax.sharding import PartitionSpec as P

K = 4
NY, NZ, NX = 4, 8, 4
DP = ("y", "zl")
MP = ("x", "zh", "core")
F32, BF16 = jnp.float32, jnp.bfloat16
NT = (((1,), (1,)), ((), ()))
TN = (((0,), (0,)), ((), ()))
SUB = 4
LAG, SKEW = 3, 2


def kernel(
    logits, targets, mask, rewards, groups, ug, mix, w_out,
    lp_out, loss_out, gmix_out, gw_out,
    LG, UV, US, GR, MX, W, G2, PF, RB, SB, GW, YS, YR, INFO, GRP, REW, WSC, LSC, STA, STB, LZ, LY,
    lsem, zsem, xsem, dsem, msem, wsem, rsem, ysem, ssem, mssem, sends,
):
    y, k, x = lax.axis_index("y"), lax.axis_index("zl"), lax.axis_index("x")
    h, c = lax.axis_index("zh"), lax.axis_index("core")
    rows, vocab = LG.shape
    depth = W.shape[2]
    xr, xl = lax.rem(x + 1, NX), lax.rem(x + NX - 1, NX)
    xo = lax.rem(x + 2, NX)
    yr, yl = lax.rem(y + 1, NY), lax.rem(y + NY - 1, NY)
    yo = lax.rem(y + 2, NY)
    right, left, opp = {"zl": k + 1}, {"zl": k - 1}, {"core": 1 - c}

    def idx(xx, cc, zz, hh):
        return ((xx * 2 + cc) * NZ + zz) * 2 + hh

    def unit(xx, cc, zz):
        return GR.at[pl.ds(idx(xx, cc, zz, 0), 2)]

    def put(src, dst, send, recv, where):
        pltpu.make_async_remote_copy(
            src_ref=src, dst_ref=dst, send_sem=send, recv_sem=recv,
            device_id=where, device_id_type=pl.DeviceIdType.MESH,
        ).start()

    def take(ref, sem):
        pltpu.make_async_copy(ref, ref, sem).wait()

    def cols(i):
        return pl.ds(pl.multiple_of(i * depth, depth), depth)

    load_rows = pltpu.make_async_copy(ug, UV, lsem.at[1])
    load_rows.start()

    barrier = pltpu.get_barrier_semaphore()
    peers = []
    for step in range(1, 2 * NZ):
        place = lax.rem(h * NZ + k + step, 2 * NZ)
        peers.append({"zh": place // NZ, "zl": lax.rem(place, NZ)})
    peers += [{"y": lax.rem(y + i, NY)} for i in range(1, NY)]
    peers += [{"x": lax.rem(x + i, NX)} for i in range(1, NX)]
    peers += [opp, {"zh": 1 - h, "core": 1 - c}]
    for peer in peers:
        pl.semaphore_signal(barrier, inc=1, device_id=peer, device_id_type=pl.DeviceIdType.MESH)

    load_w = pltpu.make_async_copy(w_out, W.at[y], lsem.at[3])
    load_w.start()
    own_rows = pl.ds(pl.multiple_of(k * rows, rows), rows)
    for q in range(SUB):
        pltpu.make_async_copy(
            mix.at[:, pl.ds(q * 128, 128)], MX.at[q, own_rows], lsem.at[2]
        ).start()
    load_logits = pltpu.make_async_copy(logits, LG, lsem.at[0])
    load_logits.start()
    for yy in range(NY):
        pltpu.make_async_copy(
            ug.at[:, cols(yy * NZ + k)],
            GR.at[idx(x, c, k, h), :, pl.ds(yy * depth, depth)], zsem.at[k],
        ).start()

    lane = lax.broadcasted_iota(jnp.int32, (1, 128), 1)
    length = jnp.sum(mask[...].astype(F32), axis=1, keepdims=True)
    facts = jnp.where(lane == 0, jnp.broadcast_to(rewards[...].astype(F32), (1, 128)), 0.0)
    facts = facts + jnp.where(lane == 1, jnp.broadcast_to(groups[...].astype(F32), (1, 128)), 0.0)
    facts = facts + jnp.where(lane == 2, jnp.broadcast_to(length, (1, 128)), 0.0)
    me = y * NZ + k
    INFO[me] = facts

    load_rows.wait()
    for zz in range(NZ):
        for yy in range(NY):
            US[zz, :, yy * depth : (yy + 1) * depth] = UV[
                :, (yy * NZ + zz) * depth : (yy * NZ + zz + 1) * depth
            ]
    pl.semaphore_wait(barrier, len(peers))

    for i in range(1, NZ):
        put(INFO.at[me], INFO.at[me], sends.at[0], ssem.at[0], {"zl": lax.rem(k + i, NZ)})
    mine = idx(x, c, k, h)
    for far in range(NZ - 1, -1, -1):
        for side in (1, -1) if far else (1,):
            to = k + side * far

            def send_rows(to=to, far=far):
                for hh in (0, 1):
                    if far == 0 and hh == 0:
                        continue
                    zh = hh if far else 1 - h
                    put(US.at[to], GR.at[mine], sends.at[1], zsem.at[k], {"zl": to, "zh": zh})

            if far == 0:
                send_rows()
            else:
                pl.when((to >= 0) & (to < NZ))(send_rows)
    half = W.shape[1] // 2
    first, second = pl.ds(0, half), pl.ds(half, half)
    load_w.wait()
    put(W.at[y, first], W.at[y, first], sends.at[2], wsem.at[0], {"y": yr})
    put(W.at[y, second], W.at[y, second], sends.at[2], wsem.at[3], {"y": yl})
    put(W.at[y, second], W.at[y, second], sends.at[2], wsem.at[1], {"y": yr})
    put(W.at[y, first], W.at[y, first], sends.at[2], wsem.at[4], {"y": yl})

    step_rows = rows // SUB

    def mix_at(zz, q):
        return MX.at[q, pl.ds(pl.multiple_of(zz * rows, rows), rows)]

    def forward(hop, q):
        for side, away, ok in ((0, -1, k < NZ - 1), (1, 1, k > 0)):
            origin = k + away * hop

            def one(side=side, origin=origin, ok=ok):
                @pl.when(hop > 0)
                def _():
                    take(mix_at(origin, q), msem.at[origin, q])

                @pl.when(ok)
                def _():
                    put(
                        mix_at(origin, q), mix_at(origin, q), mssem.at[side, hop],
                        msem.at[origin, q], (right, left)[side],
                    )

            pl.when((hop >= 0) & (hop < NZ) & (origin >= 0) & (origin < NZ))(one)

    def z_step(t):
        s = t - LAG
        going = (
            (0, NZ - 1 - (s - k), (s >= k) & (s < NZ - 1), k > 0),
            (1, s - (NZ - 1 - k), (s >= NZ - 1 - k) & (s < NZ - 1), k < NZ - 1),
        )

        def one(q, carry):
            part = pl.ds(pl.multiple_of(q * step_rows, step_rows), step_rows)
            for side, to, ok, more in going:

                def store(side=side, to=to, more=more):
                    @pl.when(more)
                    def _():
                        take(RB.at[side, to, part], rsem.at[side, to, q])
                        SB[to, part, :] = (PF[to, part, :] + RB[side, to, part, :].astype(F32)).astype(BF16)

                    @pl.when(jnp.logical_not(more))
                    def _():
                        SB[to, part, :] = PF[to, part, :].astype(BF16)

                pl.when(ok)(store)
            forward(t - SKEW * (q // 2), q)
            for side, to, ok, more in going:

                def send(side=side, to=to):
                    put(
                        SB.at[to, part], RB.at[side, to, part], sends.at[8],
                        rsem.at[side, to, q], (right, left)[side],
                    )

                pl.when(ok)(send)
            return carry

        lax.fori_loop(0, SUB, one, 0)

    take(MX.at[:, own_rows], lsem.at[2])
    z_step(0)

    load_logits.wait()
    eye = lax.broadcasted_iota(jnp.int32, (rows, rows), 0) == lax.broadcasted_iota(
        jnp.int32, (rows, rows), 1
    )
    column = lax.broadcasted_iota(jnp.int32, (rows, 128), 1).astype(F32)
    shift = ((x * 2 + h) * 2 + c) * vocab
    wanted = (targets[...] - shift).astype(F32)
    wanted = jnp.sum(jnp.where(eye, wanted, 0.0), axis=1, keepdims=True)

    def piece(j):
        return LG[:, pl.ds(pl.multiple_of(j * 128, 128), 128)].astype(F32)

    tiles = vocab // 128
    peak = lax.fori_loop(
        0, tiles, lambda j, m: jnp.maximum(m, piece(j)), jnp.full((rows, 128), -jnp.inf, F32)
    )
    peak = jnp.max(peak, axis=1, keepdims=True)

    def collect(j, carry):
        total, found = carry
        value = piece(j)
        total = total + jnp.exp(value - peak)
        at = wanted - (j * 128).astype(F32)
        return total, found + jnp.where(column == at, value, 0.0)

    zero = jnp.zeros((rows, 128), F32)
    total, found = lax.fori_loop(0, tiles, collect, (zero, zero))

    def as_row(v):
        return jnp.sum(jnp.where(eye, v, 0.0), axis=0, keepdims=True)

    a = h * 2 + c
    STA[a, 0:1, :] = as_row(peak)
    STA[a, 1:2, :] = as_row(jnp.sum(total, axis=1, keepdims=True))
    STA[a, 2:3, :] = as_row(jnp.sum(found, axis=1, keepdims=True))

    take(INFO.at[pl.ds(0, NZ - 1)], ssem.at[0])
    line = INFO.at[pl.ds(y * NZ, NZ)]
    for i in range(1, NY):
        put(line, line, sends.at[4], ssem.at[1], {"y": lax.rem(y + i, NY)})
    for peer in ({"zh": 1 - h}, opp, {"zh": 1 - h, "core": 1 - c}):
        put(STA.at[a], STA.at[a], sends.at[3], ssem.at[2], peer)

    take(W.at[yl, first], wsem.at[0])
    put(W.at[yl, first], W.at[yl, first], sends.at[5], wsem.at[2], {"y": yr})
    take(W.at[yr, second], wsem.at[3])
    put(W.at[yr, second], W.at[yr, second], sends.at[5], wsem.at[5], {"y": yl})

    def weights():
        take(INFO.at[pl.ds(0, (NY - 1) * NZ)], ssem.at[1])
        count = jnp.zeros((1, 128), F32)
        for r in range(NY * NZ):
            fact = INFO[r]
            count = count + fact
            GRP[r] = jnp.broadcast_to(fact[:, 1:2], (1, 128))
            REW[r] = jnp.broadcast_to(fact[:, 0:1], (1, 128))
        count = jnp.broadcast_to(count[:, 2:3], (1, 128))

        def weigh(zz, carry):
            reward, group = REW[y * NZ + zz], GRP[y * NZ + zz]
            own = jnp.zeros((1, 128), F32)
            for r in range(NY * NZ):
                own = own + jnp.where(GRP[r] == group, REW[r], 0.0)
            WSC[zz] = (reward - (own - reward) / (K - 1)) / count
            LSC[zz] = jnp.broadcast_to(INFO[y * NZ + zz][:, 2:3], (1, 128))
            return carry

        lax.fori_loop(0, NZ, weigh, 0)

    def merge(ref, n):
        top = ref[0, 0:1, :]
        for i in range(1, n):
            top = jnp.maximum(top, ref[i, 0:1, :])
        total = jnp.zeros_like(top)
        found = jnp.zeros_like(top)
        for i in range(n):
            total = total + ref[i, 1:2, :] * jnp.exp(ref[i, 0:1, :] - top)
            found = found + ref[i, 2:3, :]
        return top, total, found

    def join_stats():
        take(STA.at[pl.ds(0, 3)], ssem.at[2])
        for i, v in enumerate(merge(STA, 4)):
            STB[x, i : i + 1, :] = v
        for i in range(1, NX):
            put(STB.at[x], STB.at[x], sends.at[9], ssem.at[3], {"x": lax.rem(x + i, NX)})

    def arrived(zz):
        take(unit(x, c, zz), zsem.at[zz])
        here = unit(x, c, zz)
        put(here, here, sends.at[6], xsem.at[0, zz], {"x": xr})
        put(here, here, sends.at[6], xsem.at[1, zz], {"x": xl})
        put(here, here, sends.at[7], dsem.at[zz], opp)

    def passed(zz):
        for side, origin, to in ((0, xl, xr), (1, xr, xl)):
            here = unit(origin, c, zz)
            take(here, xsem.at[side, zz])
            part = GR.at[idx(origin, c, zz, side)]
            put(part, part, sends.at[6], xsem.at[2 + side, zz], {"x": to})
            put(here, here, sends.at[7], dsem.at[zz], opp)

    def closed(zz):
        for side in (0, 1):
            take(GR.at[idx(xo, c, zz, side)], xsem.at[2 + side, zz])
        here = unit(xo, c, zz)
        put(here, here, sends.at[7], dsem.at[zz], opp)

    def scaled(zz):
        take(GR.at[pl.ds(0, 8)], dsem.at[zz])
        weight, limit = WSC[zz], LSC[zz]
        base = pl.multiple_of(zz * rows, rows)

        def scale(i, carry):
            xx, hh = i // 2, lax.rem(i, 2)
            pair = jnp.concatenate(
                [GR[idx(xx, cc, zz, hh)].astype(F32) for cc in (0, 1)], axis=0
            )
            place = (lax.broadcasted_iota(jnp.int32, (16, 128), 0) + i * 16).astype(F32)
            factor = jnp.where(place < limit, -weight, 0.0)
            factor = jnp.concatenate([factor] * (pair.shape[1] // 128), axis=1)
            G2[pl.ds(pl.multiple_of(base + i * 16, 16), 16), :] = (factor * pair).astype(BF16)
            return carry

        lax.fori_loop(0, rows // 16, scale, 0)

    def partial(zz):
        block = G2[pl.ds(pl.multiple_of(zz * rows, rows), rows), :]
        acc = None
        for yy in range(NY):
            one = lax.dot_general(
                block[:, yy * depth : (yy + 1) * depth], W[yy], NT, preferred_element_type=F32
            )
            acc = one if acc is None else acc + one
        PF[zz] = acc

    def both(far, act):
        for side in (1, -1):
            zz = k + side * far
            ok = (zz >= 0) & (zz < NZ) & (far >= 0) & (far < NZ)
            if side == -1:
                ok = ok & (far > 0)

            pl.when(ok)(lambda zz=zz: act(zz))

    def lines(turn, act):
        both(NZ - 1 - 2 * turn, act)
        both(NZ - 2 - 2 * turn, act)

    def step(t, carry):
        lines(t, arrived)
        lines(t - 1, passed)
        lines(t - 2, closed)

        @pl.when(t == 2)
        def _():
            weights()
            take(W.at[yl, second], wsem.at[1])
            take(W.at[yr, first], wsem.at[4])
            take(W.at[yo, first], wsem.at[2])
            take(W.at[yo, second], wsem.at[5])

        lines(t - LAG, scaled)
        both(NZ - 1 - (t - LAG), partial)
        pl.when(t > 0)(lambda: z_step(t))
        pl.when(t == 5)(join_stats)
        return carry

    def product(q):
        value = lax.dot_general(MX[q], G2[...], TN, preferred_element_type=F32)
        for yy in range(NY):
            GW[q, yy] = value[:, yy * depth : (yy + 1) * depth]

    def stage(slot, value):
        YS[slot] = value.astype(BF16)

    def pass_on(slot, where):
        put(YS.at[slot], YR.at[slot], sends.at[11], ysem.at[slot], where)

    to_right, to_left = {"y": yr}, {"y": yl}

    def y_first(pair):
        p, q = 2 * pair, 6 * pair
        product(p)
        stage(q, GW[p, yo])
        product(p + 1)
        pass_on(q, to_right)
        stage(q + 1, GW[p + 1, yo])
        stage(q + 4, GW[p + 1, yr])
        pass_on(q + 1, to_left)
        stage(q + 5, GW[p, yl])
        pass_on(q + 4, to_right)
        pass_on(q + 5, to_left)

    def y_second(pair):
        p, q = 2 * pair, 6 * pair
        take(YR.at[q], ysem.at[q])
        stage(q + 2, GW[p, yr] + YR[q].astype(F32))
        take(YR.at[q + 1], ysem.at[q + 1])
        pass_on(q + 2, to_right)
        stage(q + 3, GW[p + 1, yl] + YR[q + 1].astype(F32))
        pass_on(q + 3, to_left)

    def y_third(pair):
        q = 6 * pair
        for p, one, two in ((2 * pair, q + 2, q + 5), (2 * pair + 1, q + 3, q + 4)):
            take(YR.at[two], ysem.at[two])
            take(YR.at[one], ysem.at[one])
            value = GW[p, y] + YR[one].astype(F32) + YR[two].astype(F32)
            gw_out[pl.ds(p * 128, 128), :] = value.astype(BF16)

    lax.fori_loop(0, NZ, step, 0)
    y_first(0)
    lax.fori_loop(NZ, NZ + 1, step, 0)
    y_second(0)

    take(STB.at[pl.ds(0, NX - 1)], ssem.at[3])
    top, total, found = merge(STB, NX)
    logprob = found - (top + jnp.log(total))
    lp_out[...] = logprob
    weight = jnp.where(lane.astype(F32) < LSC[k], WSC[k], 0.0)
    LZ[k] = jnp.broadcast_to(-jnp.sum(weight * logprob, axis=1, keepdims=True), (1, 128))

    lax.fori_loop(NZ + 1, NZ + SKEW, step, 0)
    for i in range(1, NZ):
        put(LZ.at[k], LZ.at[k], sends.at[10], ssem.at[4], {"zl": lax.rem(k + i, NZ)})
    y_first(1)
    partial(k)
    y_third(0)

    def add_side(side):
        for q in range(SUB):
            part = pl.ds(q * step_rows, step_rows)
            take(RB.at[side, k, part], rsem.at[side, k, q])
        PF[k] = PF[k] + RB[side, k].astype(F32)

    pl.when(k > 0)(lambda: add_side(0))
    pl.when(k < NZ - 1)(lambda: add_side(1))
    gmix_out[...] = PF[k].astype(BF16)

    y_second(1)
    take(LZ.at[pl.ds(0, NZ - 1)], ssem.at[4])
    LY[y] = jnp.sum(LZ[...], axis=0)
    for i in range(1, NY):
        put(LY.at[y], LY.at[y], sends.at[12], ssem.at[5], {"y": lax.rem(y + i, NY)})
    y_third(1)
    take(LY.at[pl.ds(0, NY - 1)], ssem.at[5])
    loss_out[...] = jnp.sum(LY[...], axis=0)

    take(INFO.at[pl.ds(0, NZ - 1)], sends.at[0])
    take(GR.at[pl.ds(0, 2 * NZ - 1)], sends.at[1])
    take(W.at[pl.ds(0, 2)], sends.at[2])
    take(STA.at[pl.ds(0, 3)], sends.at[3])
    take(INFO.at[pl.ds(0, (NY - 1) * NZ)], sends.at[4])
    take(W.at[0], sends.at[5])
    take(GR.at[pl.ds(0, 6 * NZ)], sends.at[6])
    take(GR.at[pl.ds(0, 8 * NZ)], sends.at[7])
    take(SB.at[pl.ds(0, NZ - 1)], sends.at[8])
    take(STB.at[pl.ds(0, NX - 1)], sends.at[9])
    take(LZ.at[pl.ds(0, NZ - 1)], sends.at[10])
    take(YR, sends.at[11])
    take(LY.at[pl.ds(0, NY - 1)], sends.at[12])
    for side, away, ok in ((0, -1, k < NZ - 1), (1, 1, k > 0)):
        for hop in range(NZ):
            origin = k + away * hop
            pl.when((origin >= 0) & (origin < NZ) & ok)(
                lambda side=side, hop=hop: take(MX.at[:, pl.ds(0, rows)], mssem.at[side, hop])
            )


def finish(lp, loss, gmix, gw, lp_out, loss_out, gmix_out, gw_out):
    lp_out[...] = lp[...]
    loss_out[0, 0] = jnp.sum(loss[:, 0:1])
    gmix_out[...] = gmix[...]
    gw_out[...] = gw[...]


def shards(logits, targets, resp_mask, rewards, groups, unit_grad, mix, w_out):
    rows, vocab = logits.shape
    heads, depth = w_out.shape
    sub = unit_grad.shape[0]
    vmem = pl.BlockSpec(memory_space=pltpu.VMEM)
    smem = pl.BlockSpec(memory_space=pltpu.SMEM)
    hbm = pl.BlockSpec(memory_space=pltpu.HBM)
    dma = pltpu.SemaphoreType.DMA
    logprob, loss, grad_mix, grad_w = pl.pallas_call(
        kernel,
        name="step",
        out_shape=(
            jax.ShapeDtypeStruct((1, rows), F32),
            jax.ShapeDtypeStruct((1, 128), F32),
            jax.ShapeDtypeStruct((rows, heads), BF16),
            jax.ShapeDtypeStruct((heads, depth), BF16),
        ),
        in_specs=[hbm, vmem, vmem, vmem, vmem, hbm, hbm, hbm],
        out_specs=(vmem, vmem, vmem, vmem),
        scratch_shapes=[
            pltpu.VMEM((rows, vocab), BF16),
            pltpu.VMEM((sub, NY * NZ * depth), BF16),
            pltpu.VMEM((NZ, sub, NY * depth), BF16),
            pltpu.VMEM((NX * 2 * NZ * 2, sub, NY * depth), BF16),
            pltpu.VMEM((SUB, NZ * rows, heads // SUB), BF16),
            pltpu.VMEM((NY, heads, depth), BF16),
            pltpu.VMEM((NZ * rows, NY * depth), BF16),
            pltpu.VMEM((NZ, rows, heads), F32),
            pltpu.VMEM((2, NZ, rows, heads), BF16),
            pltpu.VMEM((NZ, rows, heads), BF16),
            pltpu.VMEM((SUB, NY, heads // SUB, depth), F32),
            pltpu.VMEM((12, heads // SUB, depth), BF16),
            pltpu.VMEM((12, heads // SUB, depth), BF16),
            pltpu.VMEM((NY * NZ, 1, 128), F32),
            pltpu.VMEM((NY * NZ, 1, 128), F32),
            pltpu.VMEM((NY * NZ, 1, 128), F32),
            pltpu.VMEM((NZ, 1, 128), F32),
            pltpu.VMEM((NZ, 1, 128), F32),
            pltpu.VMEM((4, 8, 128), F32),
            pltpu.VMEM((NX, 8, 128), F32),
            pltpu.VMEM((NZ, 1, 128), F32),
            pltpu.VMEM((NY, 1, 128), F32),
            dma((4,)), dma((NZ,)), dma((4, NZ)), dma((NZ,)), dma((NZ, SUB)), dma((6,)),
            dma((2, NZ, SUB)), dma((12,)), dma((6,)), dma((2, NZ)), dma((13,)),
        ],
        compiler_params=pltpu.CompilerParams(
            collective_id=0, has_side_effects=True, vmem_limit_bytes=58 * 1024 * 1024
        ),
    )(
        logits, targets.reshape(1, rows), resp_mask.reshape(1, rows),
        rewards.reshape(1, 1), groups.reshape(1, 1),
        unit_grad, mix, w_out,
    )
    logprob, loss, grad_mix, grad_w = pl.pallas_call(
        finish,
        name="finish",
        out_shape=(
            jax.ShapeDtypeStruct((1, rows), F32),
            jax.ShapeDtypeStruct((1, 1), F32),
            jax.ShapeDtypeStruct((rows, heads), BF16),
            jax.ShapeDtypeStruct((heads, depth), BF16),
        ),
        in_specs=[vmem] * 4,
        out_specs=(vmem, smem, vmem, vmem),
    )(logprob, loss, grad_mix, grad_w)
    return logprob.reshape(rows), loss.reshape(()), grad_mix, grad_w


def solution(mesh):
    finer = Mesh(mesh.devices.reshape(NY, NZ, NX, 2, 2), DP + MP)
    in_specs = (
        P(DP, MP), P(DP), P(DP), P(DP), P(DP), P(DP + MP, None), P(DP, MP), P(MP, DP)
    )
    out_specs = (P(DP), P(), P(DP, MP), P(MP, DP))
    return jax.shard_map(
        shards, mesh=finer, in_specs=in_specs, out_specs=out_specs, check_vma=False
    )
```

```python
import jax
import jax.numpy as jnp
from jax import lax
from jax.experimental import pallas as pl
from jax.experimental.pallas import tpu as pltpu
from jax.sharding import Mesh
from jax.sharding import PartitionSpec as P

K = 4
NY, NZ, NX = 4, 8, 4
DP = ("y", "zl")
MP = ("x", "zh", "core")
F32, BF16 = jnp.float32, jnp.bfloat16
NT = (((1,), (1,)), ((), ()))
TN = (((0,), (0,)), ((), ()))
SUB = 4
LAG, OFF, SKEW, CUT = 3, 1, 1, 3
SCALE_AT = (3, 4, 5, 6)
JOIN_AT = 4


def kernel(
    logits, targets, mask, rewards, groups, ug, mix, w_out,
    lp_out, loss_out, gmix_out, gw_out,
    LG, UV, US, GR, MX, W, G2, PF, RB, SB, GW, YS, YR, INFO, GRP, REW, WSC, LSC, STA, STB, LZ, LY,
    lsem, zsem, xsem, dsem, msem, wsem, rsem, ysem, ssem, mssem, sends,
):
    y, k, x = lax.axis_index("y"), lax.axis_index("zl"), lax.axis_index("x")
    h, c = lax.axis_index("zh"), lax.axis_index("core")
    rows, vocab = LG.shape
    depth = W.shape[2]
    xr, xl = lax.rem(x + 1, NX), lax.rem(x + NX - 1, NX)
    xo = lax.rem(x + 2, NX)
    yr, yl = lax.rem(y + 1, NY), lax.rem(y + NY - 1, NY)
    yo = lax.rem(y + 2, NY)
    right, left, opp = {"zl": k + 1}, {"zl": k - 1}, {"core": 1 - c}

    def idx(xx, cc, zz, hh):
        return ((xx * 2 + cc) * NZ + zz) * 2 + hh

    def unit(xx, cc, zz):
        return GR.at[pl.ds(idx(xx, cc, zz, 0), 2)]

    def put(src, dst, send, recv, where):
        pltpu.make_async_remote_copy(
            src_ref=src, dst_ref=dst, send_sem=send, recv_sem=recv,
            device_id=where, device_id_type=pl.DeviceIdType.MESH,
        ).start()

    def take(ref, sem):
        pltpu.make_async_copy(ref, ref, sem).wait()

    def cols(i):
        return pl.ds(pl.multiple_of(i * depth, depth), depth)

    load_rows = pltpu.make_async_copy(ug, UV, lsem.at[1])
    load_rows.start()

    barrier = pltpu.get_barrier_semaphore()
    peers = []
    for step in range(1, 2 * NZ):
        place = lax.rem(h * NZ + k + step, 2 * NZ)
        peers.append({"zh": place // NZ, "zl": lax.rem(place, NZ)})
    peers += [{"y": lax.rem(y + i, NY)} for i in range(1, NY)]
    peers += [{"x": lax.rem(x + i, NX)} for i in range(1, NX)]
    peers += [opp, {"zh": 1 - h, "core": 1 - c}]
    for peer in peers:
        pl.semaphore_signal(barrier, inc=1, device_id=peer, device_id_type=pl.DeviceIdType.MESH)

    load_w = pltpu.make_async_copy(w_out, W.at[y], lsem.at[3])
    load_w.start()
    own_rows = pl.ds(pl.multiple_of(k * rows, rows), rows)
    for q in range(SUB):
        pltpu.make_async_copy(
            mix.at[:, pl.ds(q * 128, 128)], MX.at[q, own_rows], lsem.at[2]
        ).start()
    load_logits = pltpu.make_async_copy(logits, LG, lsem.at[0])
    load_logits.start()
    for yy in range(NY):
        pltpu.make_async_copy(
            ug.at[:, cols(yy * NZ + k)],
            GR.at[idx(x, c, k, h), :, pl.ds(yy * depth, depth)], zsem.at[k],
        ).start()

    lane = lax.broadcasted_iota(jnp.int32, (1, 128), 1)
    length = jnp.sum(mask[...].astype(F32), axis=1, keepdims=True)
    facts = jnp.where(lane == 0, jnp.broadcast_to(rewards[...].astype(F32), (1, 128)), 0.0)
    facts = facts + jnp.where(lane == 1, jnp.broadcast_to(groups[...].astype(F32), (1, 128)), 0.0)
    facts = facts + jnp.where(lane == 2, jnp.broadcast_to(length, (1, 128)), 0.0)
    me = y * NZ + k
    INFO[me] = facts

    load_rows.wait()
    for zz in range(NZ):
        for yy in range(NY):
            US[zz, :, yy * depth : (yy + 1) * depth] = UV[
                :, (yy * NZ + zz) * depth : (yy * NZ + zz + 1) * depth
            ]
    pl.semaphore_wait(barrier, len(peers))

    for i in range(1, NZ):
        put(INFO.at[me], INFO.at[me], sends.at[0], ssem.at[0], {"zl": lax.rem(k + i, NZ)})
    mine = idx(x, c, k, h)
    for far in range(NZ - 1, -1, -1):
        for side in (1, -1) if far else (1,):
            to = k + side * far

            def send_rows(to=to, far=far):
                for hh in (0, 1):
                    if far == 0 and hh == 0:
                        continue
                    zh = hh if far else 1 - h
                    put(US.at[to], GR.at[mine], sends.at[1], zsem.at[k], {"zl": to, "zh": zh})

            if far == 0:
                send_rows()
            else:
                pl.when((to >= 0) & (to < NZ))(send_rows)
    half = W.shape[1] // 2
    first, second = pl.ds(0, half), pl.ds(half, half)
    load_w.wait()
    put(W.at[y, first], W.at[y, first], sends.at[2], wsem.at[0], {"y": yr})
    put(W.at[y, second], W.at[y, second], sends.at[2], wsem.at[3], {"y": yl})
    put(W.at[y, second], W.at[y, second], sends.at[2], wsem.at[1], {"y": yr})
    put(W.at[y, first], W.at[y, first], sends.at[2], wsem.at[4], {"y": yl})

    step_rows = rows // SUB

    def mix_at(zz, q):
        return MX.at[q, pl.ds(pl.multiple_of(zz * rows, rows), rows)]

    def forward(hop, q, least):
        for side, away, ok in ((0, -1, k < NZ - 1), (1, 1, k > 0)):
            origin = k + away * hop

            def one(side=side, origin=origin, ok=ok):
                @pl.when(hop > 0)
                def _():
                    take(mix_at(origin, q), msem.at[origin, q])

                @pl.when(ok)
                def _():
                    put(
                        mix_at(origin, q), mix_at(origin, q), mssem.at[side, hop],
                        msem.at[origin, q], (right, left)[side],
                    )

            pl.when((hop >= least) & (hop < NZ) & (origin >= 0) & (origin < NZ))(one)

    def z_step(t):
        s = t - LAG
        going = (
            (0, NZ - 1 - (s - k), (s >= k) & (s < NZ - 1), k > 0),
            (1, s - (NZ - 1 - k), (s >= NZ - 1 - k) & (s < NZ - 1), k < NZ - 1),
        )

        def one(q, carry):
            part = pl.ds(pl.multiple_of(q * step_rows, step_rows), step_rows)
            for side, to, ok, more in going:

                def store(side=side, to=to, more=more):
                    @pl.when(more)
                    def _():
                        take(RB.at[side, to, part], rsem.at[side, to, q])
                        SB[to, part, :] = (PF[to, part, :] + RB[side, to, part, :].astype(F32)).astype(BF16)

                    @pl.when(jnp.logical_not(more))
                    def _():
                        SB[to, part, :] = PF[to, part, :].astype(BF16)

                pl.when(ok)(store)
            forward(t - OFF - SKEW * (q // CUT), q, 1)
            for side, to, ok, more in going:

                def send(side=side, to=to):
                    put(
                        SB.at[to, part], RB.at[side, to, part], sends.at[8],
                        rsem.at[side, to, q], (right, left)[side],
                    )

                pl.when(ok)(send)
            return carry

        lax.fori_loop(0, SUB, one, 0)

    take(MX.at[:, own_rows], lsem.at[2])
    def own(q, carry):
        forward(0, q, 0)
        return carry

    def own_blocks():
        lax.fori_loop(0, SUB, own, 0)

    own_blocks()

    load_logits.wait()
    eye = lax.broadcasted_iota(jnp.int32, (rows, rows), 0) == lax.broadcasted_iota(
        jnp.int32, (rows, rows), 1
    )
    column = lax.broadcasted_iota(jnp.int32, (rows, 128), 1).astype(F32)
    shift = ((x * 2 + h) * 2 + c) * vocab
    wanted = (targets[...] - shift).astype(F32)
    wanted = jnp.sum(jnp.where(eye, wanted, 0.0), axis=1, keepdims=True)

    def piece(j):
        return LG[:, pl.ds(pl.multiple_of(j * 128, 128), 128)].astype(F32)

    tiles = vocab // 128
    peak = lax.fori_loop(
        0, tiles, lambda j, m: jnp.maximum(m, piece(j)), jnp.full((rows, 128), -jnp.inf, F32)
    )
    peak = jnp.max(peak, axis=1, keepdims=True)

    def collect(j, carry):
        total, found = carry
        value = piece(j)
        total = total + jnp.exp(value - peak)
        at = wanted - (j * 128).astype(F32)
        return total, found + jnp.where(column == at, value, 0.0)

    zero = jnp.zeros((rows, 128), F32)
    total, found = lax.fori_loop(0, tiles, collect, (zero, zero))

    def as_row(v):
        return jnp.sum(jnp.where(eye, v, 0.0), axis=0, keepdims=True)

    a = h * 2 + c
    STA[a, 0:1, :] = as_row(peak)
    STA[a, 1:2, :] = as_row(jnp.sum(total, axis=1, keepdims=True))
    STA[a, 2:3, :] = as_row(jnp.sum(found, axis=1, keepdims=True))

    take(INFO.at[pl.ds(0, NZ - 1)], ssem.at[0])
    line = INFO.at[pl.ds(y * NZ, NZ)]
    for i in range(1, NY):
        put(line, line, sends.at[4], ssem.at[1], {"y": lax.rem(y + i, NY)})
    for peer in ({"zh": 1 - h}, opp, {"zh": 1 - h, "core": 1 - c}):
        put(STA.at[a], STA.at[a], sends.at[3], ssem.at[2], peer)

    take(W.at[yl, first], wsem.at[0])
    put(W.at[yl, first], W.at[yl, first], sends.at[5], wsem.at[2], {"y": yr})
    take(W.at[yr, second], wsem.at[3])
    put(W.at[yr, second], W.at[yr, second], sends.at[5], wsem.at[5], {"y": yl})

    def weights():
        take(INFO.at[pl.ds(0, (NY - 1) * NZ)], ssem.at[1])
        count = jnp.zeros((1, 128), F32)
        for r in range(NY * NZ):
            fact = INFO[r]
            count = count + fact
            GRP[r] = jnp.broadcast_to(fact[:, 1:2], (1, 128))
            REW[r] = jnp.broadcast_to(fact[:, 0:1], (1, 128))
        count = jnp.broadcast_to(count[:, 2:3], (1, 128))

        def weigh(zz, carry):
            reward, group = REW[y * NZ + zz], GRP[y * NZ + zz]
            own = jnp.zeros((1, 128), F32)
            for r in range(NY * NZ):
                own = own + jnp.where(GRP[r] == group, REW[r], 0.0)
            WSC[zz] = (reward - (own - reward) / (K - 1)) / count
            LSC[zz] = jnp.broadcast_to(INFO[y * NZ + zz][:, 2:3], (1, 128))
            return carry

        lax.fori_loop(0, NZ, weigh, 0)

    def merge(ref, n):
        top = ref[0, 0:1, :]
        for i in range(1, n):
            top = jnp.maximum(top, ref[i, 0:1, :])
        total = jnp.zeros_like(top)
        found = jnp.zeros_like(top)
        for i in range(n):
            total = total + ref[i, 1:2, :] * jnp.exp(ref[i, 0:1, :] - top)
            found = found + ref[i, 2:3, :]
        return top, total, found

    def join_stats():
        take(STA.at[pl.ds(0, 3)], ssem.at[2])
        for i, v in enumerate(merge(STA, 4)):
            STB[x, i : i + 1, :] = v
        for i in range(1, NX):
            put(STB.at[x], STB.at[x], sends.at[9], ssem.at[3], {"x": lax.rem(x + i, NX)})

    def arrived(zz):
        take(unit(x, c, zz), zsem.at[zz])
        here = unit(x, c, zz)
        put(here, here, sends.at[6], xsem.at[0, zz], {"x": xr})
        put(here, here, sends.at[6], xsem.at[1, zz], {"x": xl})
        put(here, here, sends.at[7], dsem.at[zz], opp)

    def passed(zz):
        for side, origin, to in ((0, xl, xr), (1, xr, xl)):
            here = unit(origin, c, zz)
            take(here, xsem.at[side, zz])
            part = GR.at[idx(origin, c, zz, side)]
            put(part, part, sends.at[6], xsem.at[2 + side, zz], {"x": to})
            put(here, here, sends.at[7], dsem.at[zz], opp)

    def closed(zz):
        for side in (0, 1):
            take(GR.at[idx(xo, c, zz, side)], xsem.at[2 + side, zz])
        here = unit(xo, c, zz)
        put(here, here, sends.at[7], dsem.at[zz], opp)

    def scaled(zz):
        take(GR.at[pl.ds(0, 8)], dsem.at[zz])
        weight, limit = WSC[zz], LSC[zz]
        base = pl.multiple_of(zz * rows, rows)

        def scale(i, carry):
            xx, hh = i // 2, lax.rem(i, 2)
            pair = jnp.concatenate(
                [GR[idx(xx, cc, zz, hh)].astype(F32) for cc in (0, 1)], axis=0
            )
            place = (lax.broadcasted_iota(jnp.int32, (16, 128), 0) + i * 16).astype(F32)
            factor = jnp.where(place < limit, -weight, 0.0)
            factor = jnp.concatenate([factor] * (pair.shape[1] // 128), axis=1)
            G2[pl.ds(pl.multiple_of(base + i * 16, 16), 16), :] = (factor * pair).astype(BF16)
            return carry

        lax.fori_loop(0, rows // 16, scale, 0)

    def partial(zz):
        block = G2[pl.ds(pl.multiple_of(zz * rows, rows), rows), :]
        acc = None
        for yy in range(NY):
            one = lax.dot_general(
                block[:, yy * depth : (yy + 1) * depth], W[yy], NT, preferred_element_type=F32
            )
            acc = one if acc is None else acc + one
        PF[zz] = acc

    def both(far, act):
        for side in (1, -1):
            zz = k + side * far
            ok = (zz >= 0) & (zz < NZ) & (far >= 0) & (far < NZ)
            if side == -1:
                ok = ok & (far > 0)

            pl.when(ok)(lambda zz=zz: act(zz))

    def lines(turn, act):
        both(NZ - 1 - 2 * turn, act)
        both(NZ - 2 - 2 * turn, act)

    def step(t, carry):
        pl.when(t == 1)(weights)
        lines(t, arrived)
        lines(t - 1, passed)
        lines(t - 2, closed)

        @pl.when(t == 2)
        def _():
            take(W.at[yl, second], wsem.at[1])
            take(W.at[yr, first], wsem.at[4])
            take(W.at[yo, first], wsem.at[2])
            take(W.at[yo, second], wsem.at[5])

        for turn, when in enumerate(SCALE_AT):
            pl.when(t == when)(lambda turn=turn: lines(turn, scaled))
        both(NZ - 1 - (t - LAG), partial)
        z_step(t)
        pl.when(t == JOIN_AT)(join_stats)
        return carry

    def product(q):
        value = lax.dot_general(MX[q], G2[...], TN, preferred_element_type=F32)
        for yy in range(NY):
            GW[q, yy] = value[:, yy * depth : (yy + 1) * depth]

    def stage(slot, value):
        YS[slot] = value.astype(BF16)

    def pass_on(slot, where):
        put(YS.at[slot], YR.at[slot], sends.at[11], ysem.at[slot], where)

    to_right, to_left = {"y": yr}, {"y": yl}

    top_half, low_half = slice(0, 64), slice(64, 128)

    def y_first(q):
        at = 6 * q
        product(q)
        stage(at, GW[q, yo, top_half])
        stage(at + 1, GW[q, yo, low_half])
        stage(at + 4, GW[q, yr, low_half])
        pass_on(at, to_right)
        pass_on(at + 1, to_left)
        stage(at + 5, GW[q, yl, top_half])
        pass_on(at + 4, to_right)
        pass_on(at + 5, to_left)

    def y_second(q):
        at = 6 * q
        take(YR.at[at], ysem.at[at])
        stage(at + 2, GW[q, yr, top_half] + YR[at].astype(F32))
        take(YR.at[at + 1], ysem.at[at + 1])
        stage(at + 3, GW[q, yl, low_half] + YR[at + 1].astype(F32))
        pass_on(at + 2, to_right)
        pass_on(at + 3, to_left)

    def y_third(q):
        at = 6 * q
        for part, one, two in ((top_half, at + 2, at + 5), (low_half, at + 3, at + 4)):
            take(YR.at[two], ysem.at[two])
            take(YR.at[one], ysem.at[one])
            value = GW[q, y, part] + YR[one].astype(F32) + YR[two].astype(F32)
            gw_out[pl.ds(q * 128 + part.start, 64), :] = value.astype(BF16)

    def finish_stats():
        take(STB.at[pl.ds(0, NX - 1)], ssem.at[3])
        top, total, found = merge(STB, NX)
        logprob = found - (top + jnp.log(total))
        lp_out[...] = logprob
        weight = jnp.where(lane.astype(F32) < LSC[k], WSC[k], 0.0)
        LZ[k] = jnp.broadcast_to(-jnp.sum(weight * logprob, axis=1, keepdims=True), (1, 128))

    def loss_over_z():
        for i in range(1, NZ):
            put(LZ.at[k], LZ.at[k], sends.at[10], ssem.at[4], {"zl": lax.rem(k + i, NZ)})

    def loss_over_y():
        take(LZ.at[pl.ds(0, NZ - 1)], ssem.at[4])
        LY[y] = jnp.sum(LZ[...], axis=0)
        for i in range(1, NY):
            put(LY.at[y], LY.at[y], sends.at[12], ssem.at[5], {"y": lax.rem(y + i, NY)})

    def add_side(side):
        for q in range(SUB):
            part = pl.ds(q * step_rows, step_rows)
            take(RB.at[side, k, part], rsem.at[side, k, q])
        PF[k] = PF[k] + RB[side, k].astype(F32)

    def close_mix():
        partial(k)
        pl.when(k > 0)(lambda: add_side(0))
        pl.when(k < NZ - 1)(lambda: add_side(1))
        gmix_out[...] = PF[k].astype(BF16)

    ready = (NZ - 1 + OFF, NZ - 1 + OFF + SKEW)
    last = max(LAG + NZ - 2, ready[1])
    early, late = range(CUT), range(CUT, SUB)
    plan = [(JOIN_AT + 2, finish_stats), (JOIN_AT + 2, loss_over_z), (last - 1, loss_over_y)]
    plan += [(ready[0], lambda q=q: y_first(q)) for q in early]
    plan += [(ready[1], lambda q=q: y_first(q)) for q in late]
    plan += [(ready[0] + 1, lambda q=q: y_second(q)) for q in early]
    plan += [(last, close_mix)]
    plan += [(ready[1] + 1, lambda q=q: y_second(q)) for q in late]
    plan += [(ready[0] + 2, lambda q=q: y_third(q)) for q in early]
    plan += [(ready[1] + 2, lambda q=q: y_third(q)) for q in late]
    at = 0
    for turn in sorted({min(when, last) for when, _ in plan}):
        lax.fori_loop(at, turn + 1, step, 0)
        at = turn + 1
        for when, act in plan:
            if min(when, last) == turn:
                act()
    take(LY.at[pl.ds(0, NY - 1)], ssem.at[5])
    loss_out[...] = jnp.sum(LY[...], axis=0)

    take(INFO.at[pl.ds(0, NZ - 1)], sends.at[0])
    take(GR.at[pl.ds(0, 2 * NZ - 1)], sends.at[1])
    take(W.at[pl.ds(0, 2)], sends.at[2])
    take(STA.at[pl.ds(0, 3)], sends.at[3])
    take(INFO.at[pl.ds(0, (NY - 1) * NZ)], sends.at[4])
    take(W.at[0], sends.at[5])
    take(GR.at[pl.ds(0, 6 * NZ)], sends.at[6])
    take(GR.at[pl.ds(0, 8 * NZ)], sends.at[7])
    take(SB.at[pl.ds(0, NZ - 1)], sends.at[8])
    take(STB.at[pl.ds(0, NX - 1)], sends.at[9])
    take(LZ.at[pl.ds(0, NZ - 1)], sends.at[10])
    take(YR, sends.at[11])
    take(LY.at[pl.ds(0, NY - 1)], sends.at[12])
    for side, away, ok in ((0, -1, k < NZ - 1), (1, 1, k > 0)):
        for hop in range(NZ):
            origin = k + away * hop
            pl.when((origin >= 0) & (origin < NZ) & ok)(
                lambda side=side, hop=hop: take(MX.at[:, pl.ds(0, rows)], mssem.at[side, hop])
            )


def finish(lp, loss, gmix, gw, lp_out, loss_out, gmix_out, gw_out):
    lp_out[...] = lp[...]
    loss_out[0, 0] = jnp.sum(loss[:, 0:1])
    gmix_out[...] = gmix[...]
    gw_out[...] = gw[...]


def shards(logits, targets, resp_mask, rewards, groups, unit_grad, mix, w_out):
    rows, vocab = logits.shape
    heads, depth = w_out.shape
    sub = unit_grad.shape[0]
    vmem = pl.BlockSpec(memory_space=pltpu.VMEM)
    smem = pl.BlockSpec(memory_space=pltpu.SMEM)
    hbm = pl.BlockSpec(memory_space=pltpu.HBM)
    dma = pltpu.SemaphoreType.DMA
    logprob, loss, grad_mix, grad_w = pl.pallas_call(
        kernel,
        name="step",
        out_shape=(
            jax.ShapeDtypeStruct((1, rows), F32),
            jax.ShapeDtypeStruct((1, 128), F32),
            jax.ShapeDtypeStruct((rows, heads), BF16),
            jax.ShapeDtypeStruct((heads, depth), BF16),
        ),
        in_specs=[hbm, vmem, vmem, vmem, vmem, hbm, hbm, hbm],
        out_specs=(vmem, vmem, vmem, vmem),
        scratch_shapes=[
            pltpu.VMEM((rows, vocab), BF16),
            pltpu.VMEM((sub, NY * NZ * depth), BF16),
            pltpu.VMEM((NZ, sub, NY * depth), BF16),
            pltpu.VMEM((NX * 2 * NZ * 2, sub, NY * depth), BF16),
            pltpu.VMEM((SUB, NZ * rows, heads // SUB), BF16),
            pltpu.VMEM((NY, heads, depth), BF16),
            pltpu.VMEM((NZ * rows, NY * depth), BF16),
            pltpu.VMEM((NZ, rows, heads), F32),
            pltpu.VMEM((2, NZ, rows, heads), BF16),
            pltpu.VMEM((NZ, rows, heads), BF16),
            pltpu.VMEM((SUB, NY, heads // SUB, depth), F32),
            pltpu.VMEM((6 * SUB, heads // SUB // 2, depth), BF16),
            pltpu.VMEM((6 * SUB, heads // SUB // 2, depth), BF16),
            pltpu.VMEM((NY * NZ, 1, 128), F32),
            pltpu.VMEM((NY * NZ, 1, 128), F32),
            pltpu.VMEM((NY * NZ, 1, 128), F32),
            pltpu.VMEM((NZ, 1, 128), F32),
            pltpu.VMEM((NZ, 1, 128), F32),
            pltpu.VMEM((4, 8, 128), F32),
            pltpu.VMEM((NX, 8, 128), F32),
            pltpu.VMEM((NZ, 1, 128), F32),
            pltpu.VMEM((NY, 1, 128), F32),
            dma((4,)), dma((NZ,)), dma((4, NZ)), dma((NZ,)), dma((NZ, SUB)), dma((6,)),
            dma((2, NZ, SUB)), dma((6 * SUB,)), dma((6,)), dma((2, NZ)), dma((13,)),
        ],
        compiler_params=pltpu.CompilerParams(
            collective_id=0, has_side_effects=True, vmem_limit_bytes=58 * 1024 * 1024
        ),
    )(
        logits, targets.reshape(1, rows), resp_mask.reshape(1, rows),
        rewards.reshape(1, 1), groups.reshape(1, 1),
        unit_grad, mix, w_out,
    )
    logprob, loss, grad_mix, grad_w = pl.pallas_call(
        finish,
        name="finish",
        out_shape=(
            jax.ShapeDtypeStruct((1, rows), F32),
            jax.ShapeDtypeStruct((1, 1), F32),
            jax.ShapeDtypeStruct((rows, heads), BF16),
            jax.ShapeDtypeStruct((heads, depth), BF16),
        ),
        in_specs=[vmem] * 4,
        out_specs=(vmem, smem, vmem, vmem),
    )(logprob, loss, grad_mix, grad_w)
    return logprob.reshape(rows), loss.reshape(()), grad_mix, grad_w


def solution(mesh):
    finer = Mesh(mesh.devices.reshape(NY, NZ, NX, 2, 2), DP + MP)
    in_specs = (
        P(DP, MP), P(DP), P(DP), P(DP), P(DP), P(DP + MP, None), P(DP, MP), P(MP, DP)
    )
    out_specs = (P(DP), P(), P(DP, MP), P(MP, DP))
    return jax.shard_map(
        shards, mesh=finer, in_specs=in_specs, out_specs=out_specs, check_vma=False
    )
```
